256 devices in a mesh: dp: 32 (over z, x_hi, core), tensor: 8 (over y, x_lo).
Axes of the slice: x: 4 (x_hi: 2, x_lo: 2; x = x_hi * 2 + x_lo), y: 4, z: 8, core: 2. Of those that a mesh axis runs over, the one named last changes fastest.
Arguments:
- hidden_in: bfloat16 [12288, 4096], P('dp'), may hold values from -6 to 6
- upstream: bfloat16 [12288, 4096], P('dp'), may hold values from -6 to 6
- merged_input_weight: bfloat16 [4096, 6144], P('dp', 'tensor'), may hold values from -0.09375 to 0.09375
- output_matrix: bfloat16 [4096, 4096], P('dp', 'tensor'), may hold values from -0.09375 to 0.09375
- norm_gain: float32 [4096], replicated, may hold values from 0.5 to 1.5
- query_gain: float32 [128], replicated, may hold values from 0.5 to 1.5
- key_gain: float32 [128], replicated, may hold values from 0.5 to 1.5
Outputs:
- hidden_grad: bfloat16 [12288, 4096], P('dp')
- input_grad: float32 [4096, 6144], P('dp', 'tensor')
- output_grad: float32 [4096, 4096], P('dp', 'tensor')
- gain_grad: float32 [4096], replicated
- query_grad: float32 [128], replicated
- key_grad: float32 [128], replicated
The draws below stay inside these ranges and needn't reach their ends.
All inputs are finite; a program needn't handle non-finite values.
Results may differ from the reference program's by a relative error of at most 0.015.
Values may be sent and summed in bfloat16 or wider, within the bound.
No kernel may reach another device: no remote copies, remote signals or barrier semaphores. Data moves between devices by JAX's collectives and lax.ppermute only.
A program may use at most 128 MiB of HBM per device.

```python
import math
from functools import partial
import jax
import jax.numpy as jnp
from jax import lax

MODEL_WIDTH = 4096
QUERY_HEADS = 32
KEY_VALUE_HEADS = 8
HEAD_SIZE = 128
SEQUENCE_LENGTH = 384
TOKENS = 12288
N_DP = 32
N_TENSOR = 8


def spiked(values, stream_key, source, target, shards_of, factor):
    def block_of(position):
        return (jnp.arange(values.shape[position]) // (values.shape[position] // shards_of)).reshape((-1,) + (1,) * (values.ndim - 1 - position))

    one_side = jax.random.permutation(stream_key, shards_of)[block_of(target)]
    second = (block_of(target) + shards_of // 2) % shards_of
    return jnp.where((block_of(source) == one_side) | (block_of(source) == second), factor * values, values)


def steps_of(key, dims, shards, least, largest):
    gain = 1.0
    for axis_at, shards_of in shards:
        steps = jax.random.uniform(jax.random.fold_in(jax.random.fold_in(key, 6), axis_at), (shards_of,), jnp.float32, least / len(shards), largest / len(shards))
        gain = gain * jnp.repeat(jnp.exp(steps), dims[axis_at] // shards_of).reshape((-1,) + (1,) * (len(dims) - 1 - axis_at))
    return gain


def gaussian(own_key, dims, spread, bound, shards=(), kind=jnp.bfloat16):
    array = jax.random.normal(own_key, dims, jnp.float32) * spread
    if len(shards) > 0:
        array = steps_of(own_key, dims, shards, -0.22, 0.18) * array
    return jnp.clip(array, min=-bound, max=bound).astype(kind)


def noise_with(stream_key, dims, scale, bound, split, heavy, held_as=jnp.bfloat16):
    drawn = scale * jax.random.normal(stream_key, dims, jnp.float32)
    if split:
        drawn = drawn * steps_of(stream_key, dims, split, -0.22, 0.18)
    return jnp.clip(spiked(drawn, jax.random.fold_in(stream_key, 3), *heavy), -bound, bound).astype(held_as)


def setup_inputs(seed: int = 0) -> dict:
    arg_keys = jax.random.split(jax.random.key(seed), 8)
    hidden_in = noise_with(arg_keys[0], (TOKENS, MODEL_WIDTH), 1.0, 6.0, ((0, 32),), (0, 1, 32, 2.75))
    upstream = noise_with(arg_keys[1], (TOKENS, MODEL_WIDTH), 1.0, 6.0, ((0, 32),), (0, 1, 32, 2.75))
    merged_input_weight = gaussian(arg_keys[2], (MODEL_WIDTH, (QUERY_HEADS + 2 * KEY_VALUE_HEADS) * HEAD_SIZE), MODEL_WIDTH ** -0.5, 0.09375, ((0, 32), (1, 8)))
    output_matrix = gaussian(arg_keys[3], (MODEL_WIDTH, QUERY_HEADS * HEAD_SIZE), (QUERY_HEADS * HEAD_SIZE) ** -0.5, 0.09375, ((0, 32), (1, 8)))
    norm_gain = jnp.clip(1.0 + 0.1 * jax.random.normal(arg_keys[4], (MODEL_WIDTH,), jnp.float32), 0.5, 1.5)
    query_gain = jnp.clip(1.0 + 0.1 * jax.random.normal(arg_keys[5], (HEAD_SIZE,), jnp.float32), 0.5, 1.5)
    key_gain = jnp.clip(1.0 + 0.1 * jax.random.normal(arg_keys[6], (HEAD_SIZE,), jnp.float32), 0.5, 1.5)
    return {"hidden_in": hidden_in, "upstream": upstream, "merged_input_weight": merged_input_weight, "output_matrix": output_matrix, "norm_gain": norm_gain, "query_gain": query_gain, "key_gain": key_gain}


EPSILON = 1e-06
ROPE_BASE = 1000000.0

def lowered_precision(value_rows):
    return lax.optimization_barrier(value_rows.astype(jnp.bfloat16))

def norm_rows(states, scaling):
    widened = states.astype(jnp.float32)
    inverse = lax.rsqrt(lax.optimization_barrier(jnp.mean(widened * widened, axis=-1, keepdims=True)) + EPSILON)
    return widened * inverse * scaling

def rope_tables(length, columns):
    half_width = columns // 2
    exponent = jnp.arange(half_width, dtype=jnp.float32) * (2.0 / columns)
    frequency = jnp.exp(-exponent * math.log(ROPE_BASE))
    places = jnp.arange(length, dtype=jnp.float32)
    angles = places[:, None] * frequency[None, :]
    return (jnp.cos(angles), jnp.sin(angles))

def head_post(projected_rows, scaling, cosine, sine):
    inverse = lax.rsqrt(lax.optimization_barrier(jnp.mean(projected_rows * projected_rows, axis=-1, keepdims=True)) + EPSILON)
    normed = projected_rows * inverse * scaling
    half_width = projected_rows.shape[-1] // 2
    layout = (projected_rows.shape[0],) + (1,) * (projected_rows.ndim - 2) + (half_width,)
    cosine_part = cosine.reshape(layout)
    sine_part = sine.reshape(layout)
    leading = normed[..., :half_width]
    trailing = normed[..., half_width:]
    return jnp.concatenate([leading * cosine_part - trailing * sine_part, trailing * cosine_part + leading * sine_part], axis=-1)

def widen(value_rows):
    return value_rows.astype(jnp.float32)

def reference(hidden_in, upstream, merged_input_weight, output_matrix, norm_gain, query_gain, key_gain):
    shard_ranks = N_TENSOR
    query_heads = QUERY_HEADS // shard_ranks
    key_head_rows = KEY_VALUE_HEADS // shard_ranks
    group_width = QUERY_HEADS // KEY_VALUE_HEADS
    attention_block = (QUERY_HEADS + 2 * KEY_VALUE_HEADS) * HEAD_SIZE // shard_ranks
    query_columns = query_heads * HEAD_SIZE
    key_columns = key_head_rows * HEAD_SIZE
    grad_scale = 1.0 / math.sqrt(TOKENS)
    score_scale = 1.0 / math.sqrt(HEAD_SIZE)
    cosine, sine = rope_tables(SEQUENCE_LENGTH, HEAD_SIZE)
    post = partial(head_post, cosine=cosine, sine=sine)
    weight_blocks = merged_input_weight.astype(jnp.float32).reshape(MODEL_WIDTH, shard_ranks, attention_block)
    causal = lax.broadcasted_iota(jnp.int32, (SEQUENCE_LENGTH, SEQUENCE_LENGTH), 0) >= lax.broadcasted_iota(jnp.int32, (SEQUENCE_LENGTH, SEQUENCE_LENGTH), 1)

    def one_sequence(carry, inputs):
        input_acc, output_acc, gain_acc, query_acc, key_acc = carry
        hidden, incoming_gradient = inputs
        local_norm, norm_back = jax.vjp(norm_rows, hidden.astype(jnp.float32), norm_gain)
        normed = lowered_precision(local_norm)
        projected_rows = jnp.dot(normed, merged_input_weight, preferred_element_type=jnp.float32).reshape(SEQUENCE_LENGTH, shard_ranks, attention_block)
        unnormed_query = projected_rows[:, :, :query_columns].reshape(SEQUENCE_LENGTH, KEY_VALUE_HEADS, group_width, HEAD_SIZE)
        unnormed_key = projected_rows[:, :, query_columns:query_columns + key_columns].reshape(SEQUENCE_LENGTH, KEY_VALUE_HEADS, HEAD_SIZE)
        value_rows = lowered_precision(projected_rows[:, :, query_columns + key_columns:].reshape(SEQUENCE_LENGTH, KEY_VALUE_HEADS, HEAD_SIZE))
        queries_full, query_back = jax.vjp(post, unnormed_query, query_gain)
        keys_full, key_back = jax.vjp(post, unnormed_key, key_gain)
        queries = lowered_precision(queries_full)
        keys = lowered_precision(keys_full)
        scores = jnp.einsum('tkgh,skh->kgts', widen(queries), widen(keys)) * score_scale
        raised = jnp.where(causal, jnp.exp(scores), 0.0)
        softmax = raised / lax.optimization_barrier(jnp.sum(raised, axis=-1, keepdims=True))
        softmax_low = lowered_precision(softmax)
        context = jnp.einsum('kgts,skh->tkgh', widen(softmax_low), widen(value_rows))
        context_low = lowered_precision(context).reshape(SEQUENCE_LENGTH, QUERY_HEADS * HEAD_SIZE)
        context_gradient = lowered_precision(jnp.dot(incoming_gradient, output_matrix, preferred_element_type=jnp.float32)).reshape(SEQUENCE_LENGTH, KEY_VALUE_HEADS, group_width, HEAD_SIZE)
        grad_probs = jnp.einsum('tkgh,skh->kgts', widen(context_gradient), widen(value_rows))
        centre = lax.optimization_barrier(jnp.sum(softmax * grad_probs, axis=-1, keepdims=True))
        grad_scores = lowered_precision(softmax * (grad_probs - centre) * score_scale)
        grad_values = jnp.einsum('kgts,tkgh->skh', widen(softmax_low), widen(context_gradient))
        grad_queries = jnp.einsum('kgts,skh->tkgh', widen(grad_scores), widen(keys))
        grad_keys = jnp.einsum('kgts,tkgh->skh', widen(grad_scores), widen(queries))
        grad_raw_query, query_part = query_back(grad_queries)
        grad_raw_key, key_part = key_back(grad_keys)
        grad_projected = lowered_precision(jnp.concatenate([grad_raw_query.reshape(SEQUENCE_LENGTH, shard_ranks, query_columns), grad_raw_key.reshape(SEQUENCE_LENGTH, shard_ranks, key_columns), grad_values.reshape(SEQUENCE_LENGTH, shard_ranks, key_columns)], axis=2).reshape(SEQUENCE_LENGTH, shard_ranks * attention_block))
        input_term = lowered_precision(jnp.dot(normed.T, grad_projected, preferred_element_type=jnp.float32) * grad_scale)
        output_term = lowered_precision(jnp.dot(incoming_gradient.T, context_low, preferred_element_type=jnp.float32) * grad_scale)
        rank_terms = jnp.einsum('trc,drc->rtd', widen(grad_projected).reshape(SEQUENCE_LENGTH, shard_ranks, attention_block), weight_blocks)
        grad_normed = lax.optimization_barrier(jnp.sum(widen(lowered_precision(rank_terms)), axis=0))
        grad_hidden, gain_part = norm_back(grad_normed)
        hidden_grad = (incoming_gradient.astype(jnp.float32) + grad_hidden).astype(jnp.bfloat16)
        carry = (input_acc + widen(input_term), output_acc + widen(output_term), gain_acc + gain_part, query_acc + query_part, key_acc + key_part)
        return (carry, hidden_grad)
    start_offset = (jnp.zeros((MODEL_WIDTH, (QUERY_HEADS + 2 * KEY_VALUE_HEADS) * HEAD_SIZE), jnp.float32), jnp.zeros((MODEL_WIDTH, QUERY_HEADS * HEAD_SIZE), jnp.float32), jnp.zeros((MODEL_WIDTH,), jnp.float32), jnp.zeros((HEAD_SIZE,), jnp.float32), jnp.zeros((HEAD_SIZE,), jnp.float32))
    sequences = (hidden_in.reshape(N_DP, SEQUENCE_LENGTH, MODEL_WIDTH), upstream.reshape(N_DP, SEQUENCE_LENGTH, MODEL_WIDTH))
    totals, hidden_parts = lax.scan(one_sequence, start_offset, sequences)
    input_grad, output_grad, gain_sum, query_sum, key_sum = totals
    return (hidden_parts.reshape(TOKENS, MODEL_WIDTH), input_grad, output_grad, gain_sum * grad_scale, query_sum * grad_scale, key_sum * grad_scale)
```

```python
import math

import jax
import jax.numpy as jnp
from jax import lax
from jax.experimental import pallas as pl
from jax.experimental.pallas import tpu as pltpu
from jax.sharding import Mesh
from jax.sharding import PartitionSpec as P

HEAD = 128
EPSILON = 1e-06
ROPE_BASE = 1000000.0
DP = ("z", "xh", "c")
TENSOR = ("y", "xl")
ORDER = (0, 1, 7, 2, 6, 3, 5, 4)
GROUPS = ((0, 3), (3, 5), (5, 7), (7, 8))
BF = jnp.bfloat16
F32 = jnp.float32
VMEM = pltpu.CompilerParams(vmem_limit_bytes=56 * 1024 * 1024)


def shift(x, axis, step):
    size = lax.axis_size(axis)
    return lax.ppermute(x, axis, [(i, (i + step) % size) for i in range(size)])


def partner(x, axis, mask):
    size = lax.axis_size(axis)
    return lax.ppermute(x, axis, [(i, i ^ mask) for i in range(size)])


def prepare_kernel(idx, hidden, upstream, gain, normed, hidden_rel, upstream_rel, inverse):
    h = hidden[...].astype(F32)
    inv = lax.rsqrt(jnp.mean(h * h, axis=-1, keepdims=True) + EPSILON)
    inverse[...] = inv
    for i in range(32):
        at = pl.ds(pl.multiple_of(idx[i] * 128, 128), 128)
        to = slice(i * 128, (i + 1) * 128)
        part = hidden[:, at]
        hidden_rel[:, to] = part
        normed[:, to] = (part.astype(F32) * inv * gain[:, at]).astype(BF)
        upstream_rel[:, to] = upstream[:, at]


def prepare(idx, hidden, upstream, gain):
    rows, width = hidden.shape
    block = 96
    full = pl.BlockSpec((block, width), lambda i, s: (i, 0))
    return pl.pallas_call(
        prepare_kernel,
        grid_spec=pltpu.PrefetchScalarGridSpec(
            num_scalar_prefetch=1,
            grid=(rows // block,),
            in_specs=[full, full, pl.BlockSpec((1, width), lambda i, s: (0, 0))],
            out_specs=[full, full, full, pl.BlockSpec((block, 1), lambda i, s: (i, 0))],
        ),
        out_shape=[
            jax.ShapeDtypeStruct((rows, width), BF),
            jax.ShapeDtypeStruct((rows, width), BF),
            jax.ShapeDtypeStruct((rows, width), BF),
            jax.ShapeDtypeStruct((rows, 1), F32),
        ],
        compiler_params=VMEM,
        name="prepare",
    )(idx, hidden, upstream, gain)


def dot_nt(a, b):
    return lax.dot_general(a, b, (((1,), (1,)), ((), ())), preferred_element_type=F32)


def dot_tn(a, b):
    return lax.dot_general(a, b, (((0,), (0,)), ((), ())), preferred_element_type=F32)


def rotated(u, gain, cosine, sine):
    inv = lax.rsqrt(jnp.mean(u * u, axis=-1, keepdims=True) + EPSILON)
    n = u * inv * gain
    return n * cosine + pltpu.roll(n, 64, 1) * sine


def probabilities(q, k, scale):
    length = q.shape[0]
    scores = dot_nt(q, k) * scale
    causal = lax.broadcasted_iota(jnp.int32, (length, length), 0) >= lax.broadcasted_iota(
        jnp.int32, (length, length), 1
    )
    raised = jnp.where(causal, jnp.exp(scores), 0.0)
    return raised / jnp.sum(raised, axis=-1, keepdims=True)


def forward_kernel(projected, query_gain, key_gain, cosine, sine, context, queries, keys, values):
    scale = 1.0 / math.sqrt(HEAD)
    heads = context.shape[1] // HEAD
    cos, sin = cosine[...], sine[...]
    k = rotated(projected[:, heads * HEAD : (heads + 1) * HEAD], key_gain[...], cos, sin).astype(BF)
    v = projected[:, (heads + 1) * HEAD :].astype(BF)
    keys[...] = k
    values[...] = v
    for h in range(heads):
        at = slice(h * HEAD, (h + 1) * HEAD)
        q = rotated(projected[:, at], query_gain[...], cos, sin).astype(BF)
        queries[:, at] = q
        p = probabilities(q, k, scale).astype(BF)
        context[:, at] = jnp.dot(p, v, preferred_element_type=F32).astype(BF)


def attend_forward(projected, query_gain, key_gain, cosine, sine):
    rows, width = projected.shape
    wide = width - 2 * HEAD
    return pl.pallas_call(
        forward_kernel,
        out_shape=[
            jax.ShapeDtypeStruct((rows, wide), BF),
            jax.ShapeDtypeStruct((rows, wide), BF),
            jax.ShapeDtypeStruct((rows, HEAD), BF),
            jax.ShapeDtypeStruct((rows, HEAD), BF),
        ],
        compiler_params=VMEM,
        name="attend_forward",
    )(projected, query_gain, key_gain, cosine, sine)


def unrotated(grad, u, gain, cosine, sine):
    d = grad * cosine + pltpu.roll(grad * sine, 64, 1)
    inv = lax.rsqrt(jnp.mean(u * u, axis=-1, keepdims=True) + EPSILON)
    plain = u * inv
    part = jnp.sum(d * plain, axis=0, keepdims=True)
    dg = d * gain
    return inv * (dg - plain * jnp.mean(plain * dg, axis=-1, keepdims=True)), part


def backward_kernel(
    projected, queries, keys, values, grad_context, query_gain, key_gain, cosine, sine,
    grad_projected, query_part, key_part,
):
    scale = 1.0 / math.sqrt(HEAD)
    heads = queries.shape[1] // HEAD
    cos, sin = cosine[...], sine[...]
    k, v = keys[...], values[...]
    grad_k = jnp.zeros(k.shape, F32)
    grad_v = jnp.zeros(v.shape, F32)
    q_part = jnp.zeros((1, HEAD), F32)
    for h in range(heads):
        at = slice(h * HEAD, (h + 1) * HEAD)
        q, d = queries[:, at], grad_context[:, at]
        p = probabilities(q, k, scale)
        dp = dot_nt(d, v)
        centre = jnp.sum(p * dp, axis=-1, keepdims=True)
        ds = (p * (dp - centre) * scale).astype(BF)
        grad_v += dot_tn(p.astype(BF), d)
        grad_k += dot_tn(ds, q)
        grad_q = jnp.dot(ds, k, preferred_element_type=F32)
        raw, part = unrotated(grad_q, projected[:, at], query_gain[...], cos, sin)
        q_part += part
        grad_projected[:, at] = raw.astype(BF)
    at = slice(heads * HEAD, (heads + 1) * HEAD)
    raw, part = unrotated(grad_k, projected[:, at], key_gain[...], cos, sin)
    grad_projected[:, at] = raw.astype(BF)
    grad_projected[:, (heads + 1) * HEAD :] = grad_v.astype(BF)
    query_part[...] = q_part
    key_part[...] = part


def attend_backward(projected, queries, keys, values, grad_context, query_gain, key_gain, cosine, sine):
    return pl.pallas_call(
        backward_kernel,
        out_shape=[
            jax.ShapeDtypeStruct(projected.shape, BF),
            jax.ShapeDtypeStruct((1, HEAD), F32),
            jax.ShapeDtypeStruct((1, HEAD), F32),
        ],
        compiler_params=VMEM,
        name="attend_backward",
    )(projected, queries, keys, values, grad_context, query_gain, key_gain, cosine, sine)


def gain_kernel(idx, grad_normed, hidden_rel, inverse, out):
    inv = inverse[...]
    for i in range(32):
        at = slice(i * 128, (i + 1) * 128)
        product = grad_normed[:, at].astype(F32) * (hidden_rel[:, at].astype(F32) * inv)
        out[pl.ds(idx[i], 1), :] = jnp.sum(product, axis=0, keepdims=True)


def gain_partial(idx, grad_normed, hidden_rel, inverse):
    return pl.pallas_call(
        gain_kernel,
        in_specs=[
            pl.BlockSpec(memory_space=pltpu.SMEM),
            pl.BlockSpec(memory_space=pltpu.VMEM),
            pl.BlockSpec(memory_space=pltpu.VMEM),
            pl.BlockSpec(memory_space=pltpu.VMEM),
        ],
        out_shape=jax.ShapeDtypeStruct((32, 128), F32),
        compiler_params=VMEM,
        name="gain_partial",
    )(idx, grad_normed, hidden_rel, inverse)


def share_kernel(idx, grad, hidden, upstream, inverse, gain, out):
    inv = inverse[...]
    plain = hidden[...].astype(F32) * inv
    total = jnp.zeros(inv.shape, F32)
    for i in range(32):
        at = slice(i * 128, (i + 1) * 128)
        natural = pl.ds(pl.multiple_of(idx[i] * 128, 128), 128)
        total += jnp.sum(grad[:, at].astype(F32) * gain[:, natural] * plain[:, at], axis=-1, keepdims=True)
    mean = total / hidden.shape[1]
    for i in range(32):
        at = slice(i * 128, (i + 1) * 128)
        natural = pl.ds(pl.multiple_of(idx[i] * 128, 128), 128)
        scaled = grad[:, at].astype(F32) * gain[:, natural]
        row = upstream[:, at].astype(F32) + inv * (scaled - plain[:, at] * mean)
        out[:, natural] = row.astype(BF)


def share_back(idx, grad, hidden, upstream, inverse, gain):
    vm = pl.BlockSpec(memory_space=pltpu.VMEM)
    return pl.pallas_call(
        share_kernel,
        in_specs=[pl.BlockSpec(memory_space=pltpu.SMEM), vm, vm, vm, vm, vm],
        out_shape=jax.ShapeDtypeStruct(grad.shape, BF),
        compiler_params=VMEM,
        name="share_back",
    )(idx, grad, hidden, upstream, inverse, gain)


def gather_rows(shard):
    rows = shard.shape[0]
    both = jnp.concatenate([shard, shift(shard, "xh", 1)], axis=0)
    right, left = {0: both}, {0: both}
    for hop in (1, 2, 3):
        right[hop] = shift(right[hop - 1], "z", 1)
        left[hop] = shift(left[hop - 1], "z", -1)
    far = jnp.concatenate(
        [shift(right[3][:rows], "z", 1), shift(left[3][rows:], "z", -1)], axis=0
    )
    groups = (
        jnp.concatenate([both, left[1], right[1]], axis=0),
        jnp.concatenate([left[2], right[2]], axis=0),
        jnp.concatenate([left[3], right[3]], axis=0),
        far,
    )
    return [(group, shift(group, "c", 1)) for group in groups]


def group_columns(array, group, half):
    first, last = GROUPS[group]
    start = half * 2048
    return array[:, start + first * 256 : start + last * 256]


def times_gathered(array, groups):
    total = None
    for g, halves in enumerate(groups):
        for half in (0, 1):
            term = jnp.dot(
                group_columns(array, g, half), halves[half], preferred_element_type=F32
            )
            total = term if total is None else total + term
    return total


def scatter_rows(left_rel, right_side, scale):
    sibling = (dot_tn(left_rel[:, 2048:], right_side) * scale).astype(BF)
    sibling = shift(sibling, "c", 1)

    def own(distance):
        at = ORDER.index(distance) * 256
        local = dot_tn(left_rel[:, at : at + 256], right_side) * scale
        return local + sibling[at : at + 256].astype(F32)

    far = own(4).astype(BF)
    a = shift(far[:128], "z", 1)
    b = shift(far[128:], "z", -1)
    three, five = own(3), own(5)
    a = jnp.concatenate([three[:128] + a.astype(F32), three[128:]], axis=0).astype(BF)
    b = jnp.concatenate([five[:128], five[128:] + b.astype(F32)], axis=0).astype(BF)
    for near, away in ((2, 6), (1, 7)):
        a = shift(a, "z", 1)
        b = shift(b, "z", -1)
        a = (own(near) + a.astype(F32)).astype(BF)
        b = (own(away) + b.astype(F32)).astype(BF)
    a = shift(a, "z", 1)
    b = shift(b, "z", -1)
    total = own(0) + a.astype(F32) + b.astype(F32)
    return total[:128] + shift(total[128:].astype(BF), "xh", 1).astype(F32)


def scatter_tokens(grad):
    y, xl = lax.axis_index("y"), lax.axis_index("xl")

    def own(distance, start=0, size=96):
        return lax.dynamic_slice_in_dim(grad, lax.rem(y + distance, 4) * 96 + start, size, 0)

    a = shift(own(2, 0, 48), "y", 1)
    b = shift(own(2, 48, 48), "y", -1)
    a = jnp.concatenate([own(1, 0, 48) + a, own(1, 48, 48)], axis=0)
    b = jnp.concatenate([own(3, 0, 48), own(3, 48, 48) + b], axis=0)
    a = shift(a, "y", 1)
    b = shift(b, "y", -1)
    total = (own(0).astype(F32) + a.astype(F32) + b.astype(F32)).astype(BF)
    other = lax.dynamic_slice_in_dim(total, (1 - xl) * 48, 48, 0)
    mine = lax.dynamic_slice_in_dim(total, xl * 48, 48, 0)
    return mine, shift(other, "xl", 1)


def gather_tokens(rows):
    y, xl = lax.axis_index("y"), lax.axis_index("xl")
    width = rows.shape[1]
    other = shift(rows, "xl", 1)
    pair = jnp.zeros((96, width), BF)
    pair = lax.dynamic_update_slice_in_dim(pair, rows, xl * 48, 0)
    pair = lax.dynamic_update_slice_in_dim(pair, other, (1 - xl) * 48, 0)
    right = shift(pair, "y", 1)
    left = shift(pair, "y", -1)
    far_a = shift(right[:48], "y", 1)
    far_b = shift(left[48:], "y", -1)
    out = jnp.zeros((384, width), BF)
    for distance, start, piece in (
        (0, 0, pair), (3, 0, right), (1, 0, left), (2, 0, far_a), (2, 48, far_b),
    ):
        out = lax.dynamic_update_slice_in_dim(out, piece, lax.rem(y + distance, 4) * 96 + start, 0)
    return out


def summed_everywhere(x):
    for axis, mask in (
        ("c", 1), ("xh", 1), ("xl", 1), ("y", 1), ("y", 2), ("z", 1), ("z", 2), ("z", 4),
    ):
        x = x + partner(x, axis, mask)
    return x


def rope_tables(length):
    half = HEAD // 2
    exponent = jnp.arange(half, dtype=F32) * (2.0 / HEAD)
    frequency = jnp.exp(-exponent * math.log(ROPE_BASE))
    angles = jnp.arange(length, dtype=F32)[:, None] * frequency[None, :]
    cosine, sine = jnp.cos(angles), jnp.sin(angles)
    return jnp.concatenate([cosine, cosine], axis=1), jnp.concatenate([-sine, sine], axis=1)


def local(hidden_in, upstream, merged_input_weight, output_matrix, norm_gain, query_gain, key_gain):
    length, width = hidden_in.shape
    grad_scale = 1.0 / math.sqrt(lax.axis_size(DP) * length)
    z, xh, c = (lax.axis_index(a) for a in DP)
    y, xl = (lax.axis_index(a) for a in TENSOR)
    pos = jnp.arange(32, dtype=jnp.int32)
    far = jnp.array(ORDER, jnp.int32)[(pos // 2) % 8]
    idx = lax.rem(z + far, 8) * 4 + (xh ^ (pos % 2)) * 2 + (c ^ (pos // 16))
    gain_row = norm_gain.reshape(1, width)
    q_gain, k_gain = query_gain.reshape(1, HEAD), key_gain.reshape(1, HEAD)
    cosine, sine = rope_tables(length)

    weight = gather_rows(merged_input_weight)
    matrix = gather_rows(output_matrix)
    normed, hidden_rel, upstream_rel, inverse = prepare(idx, hidden_in, upstream, gain_row)

    projected = times_gathered(normed, weight)
    context, queries, keys, values = attend_forward(projected, q_gain, k_gain, cosine, sine)
    grad_context = times_gathered(upstream_rel, matrix).astype(BF)
    grad_projected, query_part, key_part = attend_backward(
        projected, queries, keys, values, grad_context, q_gain, k_gain, cosine, sine
    )

    full_weight = jnp.concatenate([g[0] for g in weight] + [g[1] for g in weight], axis=0)
    grad_normed = dot_nt(grad_projected, full_weight).astype(BF)
    mine, other = scatter_tokens(grad_normed)
    grad_share = mine.astype(F32) + other.astype(F32)
    start = (y * 2 + xl) * 48
    rows = [lax.dynamic_slice_in_dim(a, start, 48, 0) for a in (hidden_rel, upstream_rel, inverse)]
    own_rows = share_back(idx, grad_share, *rows, gain_row)
    hidden_grad = gather_tokens(own_rows)

    gain_part = gain_partial(idx, grad_normed, hidden_rel, inverse)
    sums = summed_everywhere(jnp.concatenate([gain_part, query_part, key_part], axis=0)) * grad_scale

    output_grad = scatter_rows(upstream_rel, context, grad_scale)
    input_grad = scatter_rows(normed, grad_projected, grad_scale)
    return (
        hidden_grad,
        input_grad,
        output_grad,
        sums[:32].reshape(width),
        sums[32],
        sums[33],
    )


def solution(mesh):
    split = Mesh(mesh.devices.reshape(8, 2, 2, 4, 2), DP + TENSOR)
    return jax.shard_map(
        local,
        mesh=split,
        in_specs=(P(DP, None), P(DP, None), P(DP, TENSOR), P(DP, TENSOR), P(), P(), P()),
        out_specs=(P(DP, None), P(DP, TENSOR), P(DP, TENSOR), P(), P(), P()),
        check_vma=False,
    )
```

```python
import math

import jax
import jax.numpy as jnp
from jax import lax
from jax.experimental import pallas as pl
from jax.experimental.pallas import tpu as pltpu
from jax.sharding import Mesh
from jax.sharding import PartitionSpec as P

HEAD = 128
EPSILON = 1e-06
ROPE_BASE = 1000000.0
DP = ("z", "xh", "c")
TENSOR = ("y", "xl")
ORDER = (0, 1, 7, 2, 6, 3, 5, 4)
BF = jnp.bfloat16
F32 = jnp.float32
VMEM = pltpu.CompilerParams(vmem_limit_bytes=56 * 1024 * 1024)
WHOLE = pl.BlockSpec(memory_space=pltpu.VMEM)
SCALARS = pl.BlockSpec(memory_space=pltpu.SMEM)


def shift(x, axis, step):
    size = lax.axis_size(axis)
    return lax.ppermute(x, axis, [(i, (i + step) % size) for i in range(size)])


def dot(a, b):
    return jnp.dot(a, b, preferred_element_type=F32)


def dot_nt(a, b):
    return lax.dot_general(a, b, (((1,), (1,)), ((), ())), preferred_element_type=F32)


def dot_tn(a, b):
    return lax.dot_general(a, b, (((0,), (0,)), ((), ())), preferred_element_type=F32)


def block_at(i):
    return pl.ds(pl.multiple_of(i * 128, 128), 128)


def prepare_kernel(idx, hidden, upstream, gain, normed, normed_t, upstream_rel, upstream_t):
    h = hidden[...].astype(F32)
    inv = lax.rsqrt(jnp.mean(h * h, axis=-1, keepdims=True) + EPSILON)

    def step(i, _):
        at, to = block_at(idx[i]), block_at(i)
        part = (hidden[:, at].astype(F32) * inv * gain[:, at]).astype(BF)
        normed[:, to] = part
        normed_t[to, :] = part.T
        up = upstream[:, at]
        upstream_rel[:, to] = up
        upstream_t[to, :] = up.T
        return 0

    lax.fori_loop(0, 32, step, 0)


def prepare(idx, hidden, upstream, gain):
    rows, width = hidden.shape
    tall = jax.ShapeDtypeStruct((width, rows), BF)
    flat = jax.ShapeDtypeStruct((rows, width), BF)
    return pl.pallas_call(
        prepare_kernel,
        in_specs=[SCALARS, WHOLE, WHOLE, WHOLE],
        out_shape=[flat, tall, flat, tall],
        compiler_params=VMEM,
        name="prepare",
    )(idx, hidden, upstream, gain)


def project_kernel(first, wide, count, *refs):
    blocks = refs[:count]
    left = refs[count : 2 * count]
    right = refs[2 * count : 3 * count]
    out = refs[-1]
    total = None if first else refs[3 * count][...]
    p = sum(dot(left[i][...], blocks[i][:, :wide]) for i in range(count))
    u = sum(dot(right[i][...], blocks[i][:, wide:]) for i in range(count))
    out[:, :wide] = p if first else refs[3 * count][:, :wide] + p
    out[:, wide:] = u if first else refs[3 * count][:, wide:] + u


def project(total, places, blocks, normed, upstream, wide):
    rows = normed.shape[0]
    depth, width = blocks[0].shape
    columns = [pl.BlockSpec((rows, depth), lambda i, p=p: (0, p)) for p in places]
    whole = pl.BlockSpec((rows, width), lambda i: (0, 0))
    count = len(blocks)
    specs = [pl.BlockSpec((depth, width), lambda i: (0, 0))] * count + columns + columns
    args = list(blocks) + [normed] * count + [upstream] * count
    aliases = {}
    if total is not None:
        specs.append(whole)
        args.append(total)
        aliases = {3 * count: 0}

    def body(*refs):
        project_kernel(total is None, wide, count, *refs)

    return pl.pallas_call(
        body,
        grid=(1,),
        in_specs=specs,
        out_specs=whole,
        out_shape=jax.ShapeDtypeStruct((rows, width), F32),
        input_output_aliases=aliases,
        compiler_params=VMEM,
        name="project",
    )(*args)


def rotated(u, gain, cosine, sine):
    inv = lax.rsqrt(jnp.mean(u * u, axis=-1, keepdims=True) + EPSILON)
    n = u * inv * gain
    return n * cosine + pltpu.roll(n, 64, 1) * sine


def probabilities(q, k, scale):
    length = q.shape[0]
    scores = dot_nt(q, k) * scale
    causal = lax.broadcasted_iota(jnp.int32, (length, length), 0) >= lax.broadcasted_iota(
        jnp.int32, (length, length), 1
    )
    raised = jnp.where(causal, jnp.exp(scores), 0.0)
    return raised / jnp.sum(raised, axis=-1, keepdims=True)


def forward_kernel(heads, projected, query_gain, key_gain, cosine, sine, context, queries, keys, values):
    scale = 1.0 / math.sqrt(HEAD)
    cos, sin = cosine[...], sine[...]
    k = rotated(projected[:, heads * HEAD : (heads + 1) * HEAD], key_gain[...], cos, sin).astype(BF)
    v = projected[:, (heads + 1) * HEAD : (heads + 2) * HEAD].astype(BF)
    keys[...] = k
    values[...] = v
    for h in range(heads):
        at = slice(h * HEAD, (h + 1) * HEAD)
        q = rotated(projected[:, at], query_gain[...], cos, sin).astype(BF)
        queries[:, at] = q
        p = probabilities(q, k, scale).astype(BF)
        context[:, at] = dot(p, v).astype(BF)


def attend_forward(heads, projected, query_gain, key_gain, cosine, sine):
    rows = projected.shape[0]
    wide = jax.ShapeDtypeStruct((rows, heads * HEAD), BF)
    one = jax.ShapeDtypeStruct((rows, HEAD), BF)

    def body(*refs):
        forward_kernel(heads, *refs)

    return pl.pallas_call(
        body,
        out_shape=[wide, wide, one, one],
        compiler_params=VMEM,
        name="attend_forward",
    )(projected, query_gain, key_gain, cosine, sine)


def unrotated(grad, u, gain, cosine, sine):
    d = grad * cosine + pltpu.roll(grad * sine, 64, 1)
    inv = lax.rsqrt(jnp.mean(u * u, axis=-1, keepdims=True) + EPSILON)
    plain = u * inv
    part = jnp.sum(d * plain, axis=0, keepdims=True)
    dg = d * gain
    return inv * (dg - plain * jnp.mean(plain * dg, axis=-1, keepdims=True)), part


def backward_kernel(
    heads, projected, queries, keys, values, query_gain, key_gain, cosine, sine,
    grad_projected, query_part, key_part,
):
    scale = 1.0 / math.sqrt(HEAD)
    cos, sin = cosine[...], sine[...]
    k, v = keys[...], values[...]
    grad_k = jnp.zeros(k.shape, F32)
    grad_v = jnp.zeros(v.shape, F32)
    q_part = jnp.zeros((1, HEAD), F32)
    wide = (heads + 2) * HEAD
    for h in range(heads):
        at = slice(h * HEAD, (h + 1) * HEAD)
        q, d = queries[:, at], projected[:, wide + h * HEAD : wide + (h + 1) * HEAD].astype(BF)
        p = probabilities(q, k, scale)
        dp = dot_nt(d, v)
        centre = jnp.sum(p * dp, axis=-1, keepdims=True)
        ds = (p * (dp - centre) * scale).astype(BF)
        grad_v += dot_tn(p.astype(BF), d)
        grad_k += dot_tn(ds, q)
        raw, part = unrotated(dot(ds, k), projected[:, at], query_gain[...], cos, sin)
        q_part += part
        grad_projected[:, at] = raw.astype(BF)
    at = slice(heads * HEAD, (heads + 1) * HEAD)
    raw, part = unrotated(grad_k, projected[:, at], key_gain[...], cos, sin)
    grad_projected[:, at] = raw.astype(BF)
    grad_projected[:, (heads + 1) * HEAD :] = grad_v.astype(BF)
    query_part[...] = q_part
    key_part[...] = part


def attend_backward(heads, projected, queries, keys, values, query_gain, key_gain, cosine, sine):
    rows = projected.shape[0]
    part = jax.ShapeDtypeStruct((1, HEAD), F32)

    def body(*refs):
        backward_kernel(heads, *refs)

    return pl.pallas_call(
        body,
        out_shape=[jax.ShapeDtypeStruct((rows, (heads + 2) * HEAD), BF), part, part],
        compiler_params=VMEM,
        name="attend_backward",
    )(projected, queries, keys, values, query_gain, key_gain, cosine, sine)


def spread_kernel(wide, *refs):
    grad, blocks, out = refs[0][...], refs[1:-1], refs[-1]
    for i, block in enumerate(blocks):
        out[:, i * 256 : (i + 1) * 256] = dot_nt(grad, block[:, :wide]).astype(BF)


def spread(grad, blocks):
    rows, wide = grad.shape

    def body(*refs):
        spread_kernel(wide, *refs)

    return pl.pallas_call(
        body,
        out_shape=jax.ShapeDtypeStruct((rows, 256 * len(blocks)), BF),
        compiler_params=VMEM,
        name="spread",
    )(grad, *blocks)


def share_kernel(idx, grads, hidden, upstream, gain, out, part, total):
    h = hidden[...].astype(F32)
    inv = lax.rsqrt(jnp.mean(h * h, axis=-1, keepdims=True) + EPSILON)
    members = grads.shape[0]

    def first(i, row_dot):
        at, natural = block_at(i), block_at(idx[i])
        grad = grads[0, :, at].astype(F32)
        for m in range(1, members):
            grad += grads[m, :, at].astype(F32)
        plain = hidden[:, natural].astype(F32) * inv
        part[pl.ds(idx[i], 1), :] = jnp.sum(grad * plain, axis=0, keepdims=True)
        grad = grad * gain[:, natural]
        total[:, at] = grad
        return row_dot + jnp.sum(grad * plain, axis=-1, keepdims=True)

    mean = lax.fori_loop(0, 32, first, jnp.zeros(inv.shape, F32)) / hidden.shape[1]

    def second(i, _):
        at, natural = block_at(i), block_at(idx[i])
        plain = hidden[:, natural].astype(F32) * inv
        row = upstream[:, natural].astype(F32) + inv * (total[:, at] - plain * mean)
        row = row.astype(BF)
        for m in range(members):
            out[m, :, natural] = row
        return 0

    lax.fori_loop(0, 32, second, 0)


def share_back(idx, grads, hidden, upstream, gain):
    return pl.pallas_call(
        share_kernel,
        in_specs=[SCALARS, WHOLE, WHOLE, WHOLE, WHOLE],
        out_shape=[
            jax.ShapeDtypeStruct(grads.shape, BF),
            jax.ShapeDtypeStruct((32, 128), F32),
        ],
        scratch_shapes=[pltpu.VMEM(hidden.shape, F32)],
        compiler_params=VMEM,
        name="share_back",
    )(idx, grads, hidden, upstream, gain)


def sibling_terms(start, count, normed_t, upstream_t, grad_projected, context, scale):
    depth, wide, narrow = normed_t.shape[1], grad_projected.shape[1], context.shape[1]

    def body(normed, upstream, grad, ctx, out):
        out[:, :wide] = (dot(normed[...], grad[...]) * scale).astype(BF)
        out[:, wide:] = (dot(upstream[...], ctx[...]) * scale).astype(BF)

    rows = pl.BlockSpec((256, depth), lambda i: (i + start, 0))
    return pl.pallas_call(
        body,
        grid=(count,),
        in_specs=[
            rows, rows,
            pl.BlockSpec((depth, wide), lambda i: (0, 0)),
            pl.BlockSpec((depth, narrow), lambda i: (0, 0)),
        ],
        out_specs=pl.BlockSpec((256, wide + narrow), lambda i: (i, 0)),
        out_shape=jax.ShapeDtypeStruct((256 * count, wide + narrow), BF),
        compiler_params=VMEM,
        name="sibling_terms",
    )(normed_t, upstream_t, grad_projected, context)


def own_term(place, sibling, sibling_place, received, kinds, normed_t, upstream_t, grad_projected, context, scale):
    depth, wide, narrow = normed_t.shape[1], grad_projected.shape[1], context.shape[1]
    width = wide + narrow

    def body(normed, upstream, grad, ctx, sib, *refs):
        arrived, outs = refs[: len(received)], refs[len(received) :]
        for first, last, left, right in ((0, wide, normed, grad), (wide, width, upstream, ctx)):
            value = dot(left[...], right[...]) * scale + sib[:, first:last].astype(F32)
            halves = [value[:128], value[128:]]
            for (_, where), ref in zip(received, arrived):
                for h in where:
                    low = 128 * where.index(h)
                    halves[h] += ref[low : low + 128, first:last].astype(F32)
            if len(outs) == 1:
                outs[0][:128, first:last] = halves[0].astype(outs[0].dtype)
                outs[0][128:, first:last] = halves[1].astype(outs[0].dtype)
            else:
                for h in (0, 1):
                    outs[h][:, first:last] = halves[h].astype(outs[h].dtype)

    rows = pl.BlockSpec((256, depth), lambda i: (place, 0))
    specs = [
        rows, rows,
        pl.BlockSpec((depth, wide), lambda i: (0, 0)),
        pl.BlockSpec((depth, narrow), lambda i: (0, 0)),
        pl.BlockSpec((256, width), lambda i: (sibling_place, 0)),
    ] + [pl.BlockSpec(r.shape, lambda i: (0, 0)) for r, _ in received]
    size = 256 // len(kinds)
    return pl.pallas_call(
        body,
        grid=(1,),
        in_specs=specs,
        out_specs=[pl.BlockSpec((size, width), lambda i: (0, 0))] * len(kinds),
        out_shape=[jax.ShapeDtypeStruct((size, width), kind) for kind in kinds],
        compiler_params=VMEM,
        name="own_term",
    )(normed_t, upstream_t, grad_projected, context, sibling, *[r for r, _ in received])


def gathered(shard):
    rows = shard.shape[0]
    right_own = shift(shard, "z", 1)
    left_own = shift(shard, "z", -1)
    other = shift(shard, "xh", 1)
    both = jnp.concatenate([shard, other], axis=0)
    right = jnp.concatenate([right_own, shift(other, "z", 1)], axis=0)
    left = jnp.concatenate([left_own, shift(other, "z", -1)], axis=0)
    got = {0: both, 7: right, 1: left}
    for hop in (2, 3):
        right, left = shift(right, "z", 1), shift(left, "z", -1)
        got[8 - hop], got[hop] = right, left
    got[4] = jnp.concatenate([shift(right[:rows], "z", 1), shift(left[rows:], "z", -1)], axis=0)
    return got


def scattered(normed_t, upstream_t, grad_projected, context, scale):
    arrays = (normed_t, upstream_t, grad_projected, context, scale)
    early = shift(sibling_terms(13, 3, *arrays), "c", 1)
    late = shift(sibling_terms(8, 5, *arrays), "c", 1)

    def own(distance, received, kinds=(BF,)):
        place = ORDER.index(distance)
        sibling, at = (early, place - 5) if place >= 5 else (late, place)
        return own_term(place, sibling, at, received, kinds, *arrays)

    a, b = own(4, [], (BF, BF))
    a, b = shift(a, "z", 1), shift(b, "z", -1)
    (a,), (b,) = own(3, [(a, (0,))]), own(5, [(b, (1,))])
    for near, away in ((2, 6), (1, 7)):
        a, b = shift(a, "z", 1), shift(b, "z", -1)
        (a,), (b,) = own(near, [(a, (0, 1))]), own(away, [(b, (0, 1))])
    a, b = shift(a, "z", 1), shift(b, "z", -1)
    mine, other = own(0, [(a, (0, 1)), (b, (0, 1))], (F32, BF))
    return mine + shift(other, "xh", 1).astype(F32)


def exchanged(x, axes):
    return lax.all_to_all(x, axes, 0, 0, tiled=True)


def summed_everywhere(x):
    for axes in (TENSOR, ("z",), ("xh", "c")):
        members = lax.axis_size(axes)
        x = jnp.sum(exchanged(jnp.broadcast_to(x[None], (members, *x.shape)), axes), axis=0)
    return x


def rope_tables(length):
    half = HEAD // 2
    exponent = jnp.arange(half, dtype=F32) * (2.0 / HEAD)
    frequency = jnp.exp(-exponent * math.log(ROPE_BASE))
    angles = jnp.arange(length, dtype=F32)[:, None] * frequency[None, :]
    cosine, sine = jnp.cos(angles), jnp.sin(angles)
    return jnp.concatenate([cosine, cosine], axis=1), jnp.concatenate([-sine, sine], axis=1)


def local(hidden_in, upstream, merged_input_weight, output_matrix, norm_gain, query_gain, key_gain):
    length, width = hidden_in.shape
    wide = merged_input_weight.shape[1]
    heads = output_matrix.shape[1] // HEAD
    members = lax.axis_size(TENSOR)
    share = length // members
    grad_scale = 1.0 / math.sqrt(lax.axis_size(DP) * length)
    z, xh, c = (lax.axis_index(a) for a in DP)
    pos = jnp.arange(32, dtype=jnp.int32)
    far = jnp.array(ORDER, jnp.int32)[(pos // 2) % 8]
    idx = lax.rem(z + far, 8) * 4 + (xh ^ (pos % 2)) * 2 + (c ^ (pos // 16))
    gain_row = norm_gain.reshape(1, width)
    q_gain, k_gain = query_gain.reshape(1, HEAD), key_gain.reshape(1, HEAD)
    cosine, sine = rope_tables(length)

    own = gathered(jnp.concatenate([merged_input_weight, output_matrix], axis=1))
    sibling = {s: shift(block, "c", 1) for s, block in own.items()}
    normed, normed_t, upstream_rel, upstream_t = prepare(idx, hidden_in, upstream, gain_row)

    total = None
    for group in ((0,), (1, 7), (2, 6), (3, 5), (4,)):
        places = [ORDER.index(s) for s in group]
        blocks = [own[s] for s in group] + [sibling[s] for s in group]
        total = project(total, places + [8 + p for p in places], blocks, normed, upstream_rel, wide)
    context, queries, keys, values = attend_forward(heads, total, q_gain, k_gain, cosine, sine)
    grad_projected, query_part, key_part = attend_backward(
        heads, total, queries, keys, values, q_gain, k_gain, cosine, sine
    )

    grad_normed = spread(grad_projected, [own[s] for s in ORDER] + [sibling[s] for s in ORDER])
    grads = exchanged(grad_normed.reshape(members, share, width), TENSOR)
    start = lax.axis_index(TENSOR) * share
    rows = [lax.dynamic_slice_in_dim(a, start, share, 0) for a in (hidden_in, upstream)]
    own_rows, gain_part = share_back(idx, grads, *rows, gain_row)
    hidden_grad = exchanged(own_rows, TENSOR).reshape(length, width)
    sums = summed_everywhere(jnp.concatenate([gain_part, query_part, key_part], axis=0)) * grad_scale

    both = scattered(normed_t, upstream_t, grad_projected, context, grad_scale)
    return (
        hidden_grad,
        both[:, :wide],
        both[:, wide:],
        sums[:32].reshape(width),
        sums[32],
        sums[33],
    )


def solution(mesh):
    split = Mesh(mesh.devices.reshape(8, 2, 2, 4, 2), DP + TENSOR)
    return jax.shard_map(
        local,
        mesh=split,
        in_specs=(P(DP, None), P(DP, None), P(DP, TENSOR), P(DP, TENSOR), P(), P(), P()),
        out_specs=(P(DP, None), P(DP, TENSOR), P(DP, TENSOR), P(), P(), P()),
        check_vma=False,
    )
```

```python
import math

import jax
import jax.numpy as jnp
from jax import lax
from jax.experimental import pallas as pl
from jax.experimental.pallas import tpu as pltpu
from jax.sharding import Mesh
from jax.sharding import PartitionSpec as P

HEAD = 128
EPSILON = 1e-06
ROPE_BASE = 1000000.0
DP = ("z", "xh", "c")
TENSOR = ("y", "xl")
ORDER = (0, 1, 7, 2, 6, 3, 5, 4)
BF = jnp.bfloat16
F32 = jnp.float32
RATE = 2.5e9


def room(mib):
    return pltpu.CompilerParams(vmem_limit_bytes=mib * 1024 * 1024)


def lasting(micros):
    return pl.CostEstimate(flops=int(micros * RATE), bytes_accessed=1024, transcendentals=0)


WHOLE = pl.BlockSpec(memory_space=pltpu.VMEM)
SCALARS = pl.BlockSpec(memory_space=pltpu.SMEM)


def shift(x, axis, step):
    size = lax.axis_size(axis)
    return lax.ppermute(x, axis, [(i, (i + step) % size) for i in range(size)])


def dot(a, b):
    return jnp.dot(a, b, preferred_element_type=F32)


def dot_nt(a, b):
    return lax.dot_general(a, b, (((1,), (1,)), ((), ())), preferred_element_type=F32)


def dot_tn(a, b):
    return lax.dot_general(a, b, (((0,), (0,)), ((), ())), preferred_element_type=F32)


def block_at(i):
    return pl.ds(pl.multiple_of(i * 128, 128), 128)


def prepare_kernel(idx, hidden, upstream, gain, normed, normed_t, upstream_rel, upstream_t):
    h = hidden[...].astype(F32)
    inv = lax.rsqrt(jnp.mean(h * h, axis=-1, keepdims=True) + EPSILON)

    def step(i, _):
        at, to = block_at(idx[i]), block_at(i)
        part = (hidden[:, at].astype(F32) * inv * gain[:, at]).astype(BF)
        normed[:, to] = part
        normed_t[to, :] = part.T
        up = upstream[:, at]
        upstream_rel[:, to] = up
        upstream_t[to, :] = up.T
        return 0

    lax.fori_loop(0, 32, step, 0)


def prepare(idx, hidden, upstream, gain):
    rows, width = hidden.shape
    tall = jax.ShapeDtypeStruct((width, rows), BF)
    flat = jax.ShapeDtypeStruct((rows, width), BF)
    return pl.pallas_call(
        prepare_kernel,
        in_specs=[SCALARS, WHOLE, WHOLE, WHOLE],
        out_shape=[flat, tall, flat, tall],
        compiler_params=room(24),
        cost_estimate=lasting(9),
        name="prepare",
    )(idx, hidden, upstream, gain)


def project_kernel(first, wide, count, *refs):
    blocks = refs[:count]
    left = refs[count : 2 * count]
    right = refs[2 * count : 3 * count]
    out = refs[-1]
    total = None if first else refs[3 * count][...]
    p = sum(dot(left[i][...], blocks[i][:, :wide]) for i in range(count))
    u = sum(dot(right[i][...], blocks[i][:, wide:]) for i in range(count))
    out[:, :wide] = p if first else refs[3 * count][:, :wide] + p
    out[:, wide:] = u if first else refs[3 * count][:, wide:] + u


def project(total, places, blocks, normed, upstream, wide):
    rows = normed.shape[0]
    depth, width = blocks[0].shape
    columns = [pl.BlockSpec((rows, depth), lambda i, p=p: (0, p)) for p in places]
    whole = pl.BlockSpec((rows, width), lambda i: (0, 0))
    count = len(blocks)
    specs = [pl.BlockSpec((depth, width), lambda i: (0, 0))] * count + columns + columns
    args = list(blocks) + [normed] * count + [upstream] * count
    aliases = {}
    if total is not None:
        specs.append(whole)
        args.append(total)
        aliases = {3 * count: 0}

    def body(*refs):
        project_kernel(total is None, wide, count, *refs)

    return pl.pallas_call(
        body,
        grid=(1,),
        in_specs=specs,
        out_specs=whole,
        out_shape=jax.ShapeDtypeStruct((rows, width), F32),
        input_output_aliases=aliases,
        compiler_params=room(20),
        cost_estimate=lasting(1.0 * len(blocks)),
        name="project",
    )(*args)


def rotated(u, gain, cosine, sine):
    inv = lax.rsqrt(jnp.mean(u * u, axis=-1, keepdims=True) + EPSILON)
    n = u * inv * gain
    return n * cosine + pltpu.roll(n, 64, 1) * sine


def probabilities(q, k, scale):
    length = q.shape[0]
    scores = dot_nt(q, k) * scale
    causal = lax.broadcasted_iota(jnp.int32, (length, length), 0) >= lax.broadcasted_iota(
        jnp.int32, (length, length), 1
    )
    raised = jnp.where(causal, jnp.exp(scores), 0.0)
    return raised / jnp.sum(raised, axis=-1, keepdims=True)


def forward_kernel(heads, projected, query_gain, key_gain, cosine, sine, context, queries, keys, values):
    scale = 1.0 / math.sqrt(HEAD)
    cos, sin = cosine[...], sine[...]
    k = rotated(projected[:, heads * HEAD : (heads + 1) * HEAD], key_gain[...], cos, sin).astype(BF)
    v = projected[:, (heads + 1) * HEAD : (heads + 2) * HEAD].astype(BF)
    keys[...] = k
    values[...] = v

    def head(h, _):
        at = block_at(h)
        q = rotated(projected[:, at], query_gain[...], cos, sin).astype(BF)
        queries[:, at] = q
        p = probabilities(q, k, scale).astype(BF)
        context[:, at] = dot(p, v).astype(BF)
        return 0

    lax.fori_loop(0, heads, head, 0)


def attend_forward(heads, projected, query_gain, key_gain, cosine, sine):
    rows = projected.shape[0]
    wide = jax.ShapeDtypeStruct((rows, heads * HEAD), BF)
    one = jax.ShapeDtypeStruct((rows, HEAD), BF)

    def body(*refs):
        forward_kernel(heads, *refs)

    return pl.pallas_call(
        body,
        out_shape=[wide, wide, one, one],
        compiler_params=room(14),
        cost_estimate=lasting(5),
        name="attend_forward",
    )(projected, query_gain, key_gain, cosine, sine)


def unrotated(grad, u, gain, cosine, sine):
    d = grad * cosine + pltpu.roll(grad * sine, 64, 1)
    inv = lax.rsqrt(jnp.mean(u * u, axis=-1, keepdims=True) + EPSILON)
    plain = u * inv
    part = jnp.sum(d * plain, axis=0, keepdims=True)
    dg = d * gain
    return inv * (dg - plain * jnp.mean(plain * dg, axis=-1, keepdims=True)), part


def backward_kernel(
    heads, projected, queries, keys, values, query_gain, key_gain, cosine, sine,
    grad_projected, query_part, key_part, grad_k, grad_v,
):
    scale = 1.0 / math.sqrt(HEAD)
    cos, sin = cosine[...], sine[...]
    k, v = keys[...], values[...]
    grad_k[...] = jnp.zeros(grad_k.shape, F32)
    grad_v[...] = jnp.zeros(grad_v.shape, F32)
    query_part[...] = jnp.zeros(query_part.shape, F32)

    def head(h, _):
        at = block_at(h)
        q, d = queries[:, at], projected[:, block_at(heads + 2 + h)].astype(BF)
        p = probabilities(q, k, scale)
        dp = dot_nt(d, v)
        centre = jnp.sum(p * dp, axis=-1, keepdims=True)
        ds = (p * (dp - centre) * scale).astype(BF)
        grad_v[...] += dot_tn(p.astype(BF), d)
        grad_k[...] += dot_tn(ds, q)
        raw, part = unrotated(dot(ds, k), projected[:, at], query_gain[...], cos, sin)
        query_part[...] += part
        grad_projected[:, at] = raw.astype(BF)
        return 0

    lax.fori_loop(0, heads, head, 0)
    at = slice(heads * HEAD, (heads + 1) * HEAD)
    raw, part = unrotated(grad_k[...], projected[:, at], key_gain[...], cos, sin)
    grad_projected[:, at] = raw.astype(BF)
    grad_projected[:, (heads + 1) * HEAD :] = grad_v[...].astype(BF)
    key_part[...] = part


def attend_backward(heads, projected, queries, keys, values, query_gain, key_gain, cosine, sine):
    rows = projected.shape[0]
    part = jax.ShapeDtypeStruct((1, HEAD), F32)

    def body(*refs):
        backward_kernel(heads, *refs)

    return pl.pallas_call(
        body,
        out_shape=[jax.ShapeDtypeStruct((rows, (heads + 2) * HEAD), BF), part, part],
        scratch_shapes=[pltpu.VMEM((rows, HEAD), F32), pltpu.VMEM((rows, HEAD), F32)],
        compiler_params=room(18),
        cost_estimate=lasting(7),
        name="attend_backward",
    )(projected, queries, keys, values, query_gain, key_gain, cosine, sine)


def spread_kernel(wide, idx, grad, normed, gain, *refs):
    blocks, out, part = refs[:-2], refs[-2], refs[-1]
    for i, block in enumerate(blocks):
        at = slice(i * 256, (i + 1) * 256)
        value = dot_nt(grad[...], block[:, :wide])
        out[:, at] = value.astype(BF)
        sums = jnp.sum(value * normed[:, at].astype(F32), axis=0, keepdims=True)
        for j in (0, 1):
            natural = idx[2 * i + j]
            part[pl.ds(natural, 1), :] = sums[:, j * 128 : (j + 1) * 128] / gain[:, block_at(natural)]


def spread(idx, grad, normed, gain, blocks):
    rows, wide = grad.shape

    def body(*refs):
        spread_kernel(wide, *refs)

    return pl.pallas_call(
        body,
        in_specs=[SCALARS] + [WHOLE] * (3 + len(blocks)),
        out_shape=[
            jax.ShapeDtypeStruct((rows, 256 * len(blocks)), BF),
            jax.ShapeDtypeStruct((32, 128), F32),
        ],
        compiler_params=room(24),
        cost_estimate=lasting(8),
        name="spread",
    )(idx, grad, normed, gain, *blocks)


def share_kernel(idx, grads, hidden, upstream, gain, out, total):
    h = hidden[...].astype(F32)
    inv = lax.rsqrt(jnp.mean(h * h, axis=-1, keepdims=True) + EPSILON)
    members = grads.shape[0]

    def first(j, products):
        for i in range(8):
            at, natural = block_at(j * 8 + i), block_at(idx[j * 8 + i])
            grad = grads[0, :, at].astype(F32)
            for m in range(1, members):
                grad += grads[m, :, at].astype(F32)
            plain = hidden[:, natural].astype(F32) * inv
            grad = grad * gain[:, natural]
            total[:, natural] = grad
            products += grad * plain
        return products

    products = lax.fori_loop(0, 4, first, jnp.zeros((hidden.shape[0], 128), F32))
    mean = jnp.sum(products, axis=-1, keepdims=True) / hidden.shape[1]

    def second(i, _):
        at = pl.ds(pl.multiple_of(i * 512, 512), 512)
        plain = hidden[:, at].astype(F32) * inv
        row = upstream[:, at].astype(F32) + inv * (total[:, at] - plain * mean)
        row = row.astype(BF)
        for m in range(members):
            out[m, :, at] = row
        return 0

    lax.fori_loop(0, 8, second, 0)


def share_back(idx, grads, hidden, upstream, gain):
    return pl.pallas_call(
        share_kernel,
        in_specs=[SCALARS, WHOLE, WHOLE, WHOLE, WHOLE],
        out_shape=jax.ShapeDtypeStruct(grads.shape, BF),
        scratch_shapes=[pltpu.VMEM(hidden.shape, F32)],
        compiler_params=room(12),
        cost_estimate=lasting(4),
        name="share_back",
    )(idx, grads, hidden, upstream, gain)


def sibling_terms(start, count, normed_t, upstream_t, grad_projected, context, scale):
    depth, wide, narrow = normed_t.shape[1], grad_projected.shape[1], context.shape[1]

    def body(normed, upstream, grad, ctx, out):
        out[:, :wide] = (dot(normed[...], grad[...]) * scale).astype(BF)
        out[:, wide:] = (dot(upstream[...], ctx[...]) * scale).astype(BF)

    rows = pl.BlockSpec((256, depth), lambda i: (i + start, 0))
    return pl.pallas_call(
        body,
        grid=(count,),
        in_specs=[
            rows, rows,
            pl.BlockSpec((depth, wide), lambda i: (0, 0)),
            pl.BlockSpec((depth, narrow), lambda i: (0, 0)),
        ],
        out_specs=pl.BlockSpec((256, wide + narrow), lambda i: (i, 0)),
        out_shape=jax.ShapeDtypeStruct((256 * count, wide + narrow), BF),
        compiler_params=room(12),
        cost_estimate=lasting(1.0 * count),
        name="sibling_terms",
    )(normed_t, upstream_t, grad_projected, context)


def own_term(place, sibling, sibling_place, received, kinds, normed_t, upstream_t, grad_projected, context, scale):
    depth, wide, narrow = normed_t.shape[1], grad_projected.shape[1], context.shape[1]
    width = wide + narrow

    def body(normed, upstream, grad, ctx, sib, *refs):
        arrived, outs = refs[: len(received)], refs[len(received) :]
        for first, last, left, right in ((0, wide, normed, grad), (wide, width, upstream, ctx)):
            value = dot(left[...], right[...]) * scale + sib[:, first:last].astype(F32)
            halves = [value[:128], value[128:]]
            for (_, where), ref in zip(received, arrived):
                for h in where:
                    low = 128 * where.index(h)
                    halves[h] += ref[low : low + 128, first:last].astype(F32)
            if len(outs) == 1:
                outs[0][:128, first:last] = halves[0].astype(outs[0].dtype)
                outs[0][128:, first:last] = halves[1].astype(outs[0].dtype)
            else:
                for h in (0, 1):
                    outs[h][:, first:last] = halves[h].astype(outs[h].dtype)

    rows = pl.BlockSpec((256, depth), lambda i: (place, 0))
    specs = [
        rows, rows,
        pl.BlockSpec((depth, wide), lambda i: (0, 0)),
        pl.BlockSpec((depth, narrow), lambda i: (0, 0)),
        pl.BlockSpec((256, width), lambda i: (sibling_place, 0)),
    ] + [pl.BlockSpec(r.shape, lambda i: (0, 0)) for r, _ in received]
    size = 256 // len(kinds)
    return pl.pallas_call(
        body,
        grid=(1,),
        in_specs=specs,
        out_specs=[pl.BlockSpec((size, width), lambda i: (0, 0))] * len(kinds),
        out_shape=[jax.ShapeDtypeStruct((size, width), kind) for kind in kinds],
        compiler_params=room(10),
        cost_estimate=lasting(1.5),
        name="own_term",
    )(normed_t, upstream_t, grad_projected, context, sibling, *[r for r, _ in received])


def joined(mine, received, wide):
    def body(a, b, left, right):
        left[...] = a[:, :wide] + b[:, :wide].astype(F32)
        right[...] = a[:, wide:] + b[:, wide:].astype(F32)

    rows, width = mine.shape
    return pl.pallas_call(
        body,
        out_shape=[
            jax.ShapeDtypeStruct((rows, wide), F32),
            jax.ShapeDtypeStruct((rows, width - wide), F32),
        ],
        compiler_params=room(6),
        cost_estimate=lasting(1.0),
        name="joined",
    )(mine, received)


def gathered(shard):
    rows = shard.shape[0]
    right_own = shift(shard, "z", 1)
    left_own = shift(shard, "z", -1)
    other = shift(shard, "xh", 1)
    both = jnp.concatenate([shard, other], axis=0)
    right = jnp.concatenate([right_own, shift(other, "z", 1)], axis=0)
    left = jnp.concatenate([left_own, shift(other, "z", -1)], axis=0)
    got = {0: both, 7: right, 1: left}
    for hop in (2, 3):
        right, left = shift(right, "z", 1), shift(left, "z", -1)
        got[8 - hop], got[hop] = right, left
    got[4] = jnp.concatenate([shift(right[:rows], "z", 1), shift(left[rows:], "z", -1)], axis=0)
    return got


def scattered(normed_t, upstream_t, grad_projected, context, scale):
    arrays = (normed_t, upstream_t, grad_projected, context, scale)
    early = shift(sibling_terms(13, 3, *arrays), "c", 1)
    late = shift(sibling_terms(8, 5, *arrays), "c", 1)

    def own(distance, received, kinds=(BF,)):
        place = ORDER.index(distance)
        sibling, at = (early, place - 5) if place >= 5 else (late, place)
        return own_term(place, sibling, at, received, kinds, *arrays)

    a, b = own(4, [], (BF, BF))
    a, b = shift(a, "z", 1), shift(b, "z", -1)
    (a,), (b,) = own(3, [(a, (0,))]), own(5, [(b, (1,))])
    for near, away in ((2, 6), (1, 7)):
        a, b = shift(a, "z", 1), shift(b, "z", -1)
        (a,), (b,) = own(near, [(a, (0, 1))]), own(away, [(b, (0, 1))])
    a, b = shift(a, "z", 1), shift(b, "z", -1)
    mine, other = own(0, [(a, (0, 1)), (b, (0, 1))], (F32, BF))
    return joined(mine, shift(other, "xh", 1), grad_projected.shape[1])


def exchanged(x, axes):
    return lax.all_to_all(x, axes, 0, 0, tiled=True)


def summed_everywhere(x):
    for axes in (TENSOR, ("z", "xh")):
        members = lax.axis_size(axes)
        x = jnp.sum(exchanged(jnp.broadcast_to(x[None], (members, *x.shape)), axes), axis=0)
    return x + shift(x, "c", 1)


def rope_tables(length):
    half = HEAD // 2
    exponent = jnp.arange(half, dtype=F32) * (2.0 / HEAD)
    frequency = jnp.exp(-exponent * math.log(ROPE_BASE))
    angles = jnp.arange(length, dtype=F32)[:, None] * frequency[None, :]
    cosine, sine = jnp.cos(angles), jnp.sin(angles)
    return jnp.concatenate([cosine, cosine], axis=1), jnp.concatenate([-sine, sine], axis=1)


def local(hidden_in, upstream, merged_input_weight, output_matrix, norm_gain, query_gain, key_gain):
    length, width = hidden_in.shape
    wide = merged_input_weight.shape[1]
    heads = output_matrix.shape[1] // HEAD
    members = lax.axis_size(TENSOR)
    share = length // members
    grad_scale = 1.0 / math.sqrt(lax.axis_size(DP) * length)
    z, xh, c = (lax.axis_index(a) for a in DP)
    pos = jnp.arange(32, dtype=jnp.int32)
    far = jnp.array(ORDER, jnp.int32)[(pos // 2) % 8]
    idx = lax.rem(z + far, 8) * 4 + (xh ^ (pos % 2)) * 2 + (c ^ (pos // 16))
    gain_row = norm_gain.reshape(1, width)
    q_gain, k_gain = query_gain.reshape(1, HEAD), key_gain.reshape(1, HEAD)
    cosine, sine = rope_tables(length)

    own = gathered(jnp.concatenate([merged_input_weight, output_matrix], axis=1))
    sibling = {s: shift(block, "c", 1) for s, block in own.items()}
    normed, normed_t, upstream_rel, upstream_t = prepare(idx, hidden_in, upstream, gain_row)

    total = None
    for group in ((0,), (1, 7), (2, 6), (3, 5), (4,)):
        places = [ORDER.index(s) for s in group]
        blocks = [own[s] for s in group] + [sibling[s] for s in group]
        total = project(total, places + [8 + p for p in places], blocks, normed, upstream_rel, wide)
    context, queries, keys, values = attend_forward(heads, total, q_gain, k_gain, cosine, sine)
    grad_projected, query_part, key_part = attend_backward(
        heads, total, queries, keys, values, q_gain, k_gain, cosine, sine
    )

    blocks = [own[s] for s in ORDER] + [sibling[s] for s in ORDER]
    grad_normed, gain_part = spread(idx, grad_projected, normed, gain_row, blocks)
    grads = exchanged(grad_normed.reshape(members, share, width), TENSOR)
    start = lax.axis_index(TENSOR) * share
    rows = [lax.dynamic_slice_in_dim(a, start, share, 0) for a in (hidden_in, upstream)]
    own_rows = share_back(idx, grads, *rows, gain_row)
    hidden_grad = exchanged(own_rows, TENSOR).reshape(length, width)
    sums = summed_everywhere(jnp.concatenate([gain_part, query_part, key_part], axis=0)) * grad_scale

    input_grad, output_grad = scattered(normed_t, upstream_t, grad_projected, context, grad_scale)
    return (
        hidden_grad,
        input_grad,
        output_grad,
        sums[:32].reshape(width),
        sums[32],
        sums[33],
    )


def solution(mesh):
    split = Mesh(mesh.devices.reshape(8, 2, 2, 4, 2), DP + TENSOR)
    return jax.shard_map(
        local,
        mesh=split,
        in_specs=(P(DP, None), P(DP, None), P(DP, TENSOR), P(DP, TENSOR), P(), P(), P()),
        out_specs=(P(DP, None), P(DP, TENSOR), P(DP, TENSOR), P(), P(), P()),
        check_vma=False,
    )
```
